256 devices in a mesh: gx: 8 (over x_hi, y), gy: 4 (over x_lo, core), gz: 8 (over z).
Axes of the slice: x: 4 (x_hi: 2, x_lo: 2; x = x_hi * 2 + x_lo), y: 4, z: 8, core: 2. Of those that a mesh axis runs over, the one named last changes fastest.
Arguments:
- node_latents: bfloat16 [262144, 128], P(('gx', 'gy', 'gz')), may hold values from -300 to 300
- cluster_latents: bfloat16 [65536, 128], P(('gx', 'gy', 'gz')), may hold values from -6 to 6
- senders: int32 [8192, 128], P(('gx', 'gy', 'gz')), may hold values from 0 to 4095
- membership: int32 [262144], P(('gx', 'gy', 'gz')), may hold values from 0 to 255
- w_key: bfloat16 [128, 128], replicated, may hold values from -1 to 1
- w_value: bfloat16 [128, 128], replicated, may hold values from -0.5 to 0.5
- w_edge_in: bfloat16 [256, 128], replicated, may hold values from -0.375 to 0.375
- w_edge_out: bfloat16 [128, 128], replicated, may hold values from -0.5 to 0.5
- w_node_in: bfloat16 [512, 128], replicated, may hold values from -0.25 to 0.25
- w_node_out: bfloat16 [128, 128], replicated, may hold values from -0.5 to 0.5
- out_gain: float32 [128], replicated, may hold values from 0.5 to 1.5
Outputs:
- new_latents: bfloat16 [262144, 128], P(('gx', 'gy', 'gz'))
The draws below stay inside these ranges and needn't reach their ends.
All inputs are finite; a program needn't handle non-finite values.
Results may differ from the reference program's by a relative error of at most 0.005.
Values may be sent and summed in bfloat16 or wider, within the bound.
A program may use at most 64 MiB of HBM per device.

```python
import jax
import jax.numpy as jnp
from jax import lax

H = 128
NODES_DEV = 1024
CL_DEV = 256
BND = 512
DEG = 4
EDGE_ROWS = 32
NODES = 262144
CLUSTERS = 65536
N_GX = 8
N_GY = 4
N_GZ = 8
DEVICES = 256


def shared_parts(key):
    cluster_key, weight_key = jax.random.split(jax.random.fold_in(key, 7))
    clusters = jnp.clip(jax.random.normal(cluster_key, (CLUSTERS, H), jnp.float32), -6.0, 6.0)
    weights = jnp.clip(jax.random.normal(weight_key, (H, H), jnp.float32), -6.0, 6.0) / jnp.sqrt(jnp.float32(H))
    return (clusters, weights)


def draw_cluster_latents(key, part):
    return shared_parts(key)[0].astype(jnp.bfloat16)


def draw_w_key(key, part):
    return shared_parts(key)[1].astype(jnp.bfloat16)


def draw_node_latents(key, part):
    base_key = jax.random.fold_in(key, 11)
    latents = jnp.clip(jax.random.normal(base_key, (NODES, H), jnp.float32), -6.0, 6.0)
    return latents.astype(jnp.bfloat16)


def plant(drawn, own_key, least, top_value):
    longest = drawn.shape.index(max(drawn.shape))
    spots = []
    for shift in (0, 1):
        where = [jax.random.randint(jax.random.fold_in(own_key, axis), (), 0, length) for axis, length in enumerate(drawn.shape)]
        where[longest] = (where[longest] + shift) % drawn.shape[longest]
        spots.append(tuple(where))
    return drawn.at[spots[0]].set(least).at[spots[1]].set(top_value)


def normal_values(rng, shape, scale, bound, kind=jnp.bfloat16):
    return jnp.clip(scale * jax.random.normal(rng, shape, jnp.float32), -bound, bound).astype(kind)


def setup_inputs(seed: int = 0) -> dict:
    splits = jax.random.split(jax.random.key(seed), 12)
    node_latents = draw_node_latents(jax.random.fold_in(splits[11], 71), 0)
    cluster_latents = draw_cluster_latents(jax.random.fold_in(splits[11], 71), 0)
    senders = plant(jax.random.randint(splits[2], (DEVICES * EDGE_ROWS, 128), 0, NODES_DEV + 6 * BND), jax.random.fold_in(splits[2], 1), 0, (NODES_DEV + 6 * BND) - 1).astype(jnp.int32)
    membership = plant(jax.random.randint(splits[3], (NODES,), 0, CL_DEV), jax.random.fold_in(splits[3], 1), 0, CL_DEV - 1).astype(jnp.int32)
    w_key = draw_w_key(jax.random.fold_in(splits[11], 71), 0)
    w_value = normal_values(splits[5], (H, H), H ** -0.5, 0.5)
    w_edge_in = normal_values(splits[6], (2 * H, H), (2 * H) ** -0.5, 0.375)
    w_edge_out = normal_values(splits[7], (H, H), H ** -0.5, 0.5)
    w_node_in = normal_values(splits[8], (4 * H, H), (4 * H) ** -0.5, 0.25)
    w_node_out = normal_values(splits[9], (H, H), H ** -0.5, 0.5)
    out_gain = jnp.clip(1.0 + 0.1 * jax.random.normal(splits[10], (H,), jnp.float32), 0.5, 1.5)
    return dict(node_latents=node_latents, cluster_latents=cluster_latents, senders=senders, membership=membership, w_key=w_key, w_value=w_value, w_edge_in=w_edge_in, w_edge_out=w_edge_out, w_node_in=w_node_in, w_node_out=w_node_out, out_gain=out_gain)


def project(latent_rows, weight):
    return jnp.dot(latent_rows, weight, preferred_element_type=jnp.float32).astype(jnp.bfloat16)

def attend(queries, key_rows, value_rows):
    scores = jnp.dot(queries, key_rows.T, preferred_element_type=jnp.float32) / jnp.sqrt(jnp.float32(queries.shape[1]))
    highest = lax.optimization_barrier(jnp.max(scores, axis=1, keepdims=True))
    exponent = jnp.exp(scores - highest)
    numer = jnp.dot(exponent.astype(jnp.bfloat16), value_rows, preferred_element_type=jnp.float32)
    return numer / lax.optimization_barrier(jnp.sum(exponent, axis=1, keepdims=True))

def reference(node_latents, cluster_latents, senders, membership, w_key, w_value, w_edge_in, w_edge_out, w_node_in, w_node_out, out_gain):
    width = node_latents.shape[1]
    key_grid = project(cluster_latents, w_key).reshape(N_GX, N_GY, N_GZ, CL_DEV, width)
    value_grid = project(cluster_latents, w_value).reshape(N_GX, N_GY, N_GZ, CL_DEV, width)
    cluster_grid = cluster_latents.reshape(N_GX, N_GY, N_GZ, CL_DEV, width)
    node_grid = node_latents.reshape(N_GX, N_GY, N_GZ, NODES_DEV, width)
    border = node_grid[:, :, :, :BND]
    faces = jnp.stack([jnp.roll(border, 1, axis=0), jnp.roll(border, -1, axis=0), jnp.roll(border, 1, axis=1), jnp.roll(border, -1, axis=1), jnp.roll(border, 1, axis=2), jnp.roll(border, -1, axis=2)], axis=3)
    faces = faces.reshape(N_GX, N_GY, N_GZ, 6 * BND, width)
    edge_grid = senders.reshape(N_GX, N_GY, N_GZ, NODES_DEV * DEG)
    member_grid = membership.reshape(N_GX, N_GY, N_GZ, NODES_DEV)

    def one_block(device_flat):
        index_x = device_flat // (N_GY * N_GZ)
        index_y = device_flat // N_GZ % N_GY
        index_z = device_flat % N_GZ
        own = node_grid[index_x, index_y, index_z]
        pooled = attend(own, key_grid[:, index_y, index_z].reshape(-1, width), value_grid[:, index_y, index_z].reshape(-1, width))
        pooled = pooled + attend(own, key_grid[index_x, :, index_z].reshape(-1, width), value_grid[index_x, :, index_z].reshape(-1, width))
        pooled = pooled + attend(own, key_grid[index_x, index_y].reshape(-1, width), value_grid[index_x, index_y].reshape(-1, width))
        attended = (pooled * lax.rsqrt(lax.optimization_barrier(jnp.mean(pooled * pooled, axis=1, keepdims=True)) + 1e-06)).astype(jnp.bfloat16)
        extended = jnp.concatenate([own, faces[index_x, index_y, index_z]], axis=0)
        sender_rows = jnp.take(extended, edge_grid[index_x, index_y, index_z], axis=0)
        receiver_part = jnp.dot(own, w_edge_in[:width], preferred_element_type=jnp.float32)
        sender_part = jnp.dot(sender_rows, w_edge_in[width:], preferred_element_type=jnp.float32)
        edge_hidden = jax.nn.silu(sender_part.reshape(NODES_DEV, DEG, width) + receiver_part[:, None, :]).astype(jnp.bfloat16)
        messages = jnp.dot(edge_hidden.reshape(NODES_DEV * DEG, width), w_edge_out, preferred_element_type=jnp.float32)
        aggregated = lax.optimization_barrier(jnp.sum(messages.reshape(NODES_DEV, DEG, width), axis=1)).astype(jnp.bfloat16)
        own_cluster = jnp.take(cluster_grid[index_x, index_y, index_z], member_grid[index_x, index_y, index_z], axis=0)
        preact = jnp.dot(own, w_node_in[:width], preferred_element_type=jnp.float32)
        preact = preact + jnp.dot(aggregated, w_node_in[width:2 * width], preferred_element_type=jnp.float32)
        preact = preact + jnp.dot(attended, w_node_in[2 * width:3 * width], preferred_element_type=jnp.float32)
        preact = preact + jnp.dot(own_cluster, w_node_in[3 * width:], preferred_element_type=jnp.float32)
        node_hidden = jax.nn.silu(preact).astype(jnp.bfloat16)
        update = jnp.dot(node_hidden, w_node_out, preferred_element_type=jnp.float32)
        centred = update - lax.optimization_barrier(jnp.mean(update, axis=1, keepdims=True))
        variance = lax.optimization_barrier(jnp.mean(centred * centred, axis=1, keepdims=True))
        normed = centred * lax.rsqrt(variance + 1e-05)
        return (own.astype(jnp.float32) + normed * out_gain).astype(jnp.bfloat16)
    blocks = lax.map(one_block, jnp.arange(N_GX * N_GY * N_GZ, dtype=jnp.int32))
    return blocks.reshape(-1, width)
```

```python
import functools
import math

import jax
import jax.numpy as jnp
from jax import lax
from jax.experimental import pallas as pl
from jax.experimental.pallas import tpu as pltpu
from jax.sharding import PartitionSpec as P

MESH = pl.DeviceIdType.MESH
F32 = jnp.float32
BF16 = jnp.bfloat16
ROWS = 256
NT = (((1,), (1,)), ((), ()))


def dot(a, b):
    return jnp.dot(a, b, preferred_element_type=F32)


def silu(x):
    half = 0.5 * x
    return half * jnp.tanh(half) + half


def kernel(
    nodes_h, clusters_h, senders, members, wk_h, wv_h, wei_h, weo_h, wni_h, wno_h, gain_h,
    out_h,
    nodes, clusters, wk, wv, wei, weo, wni, wno, gain,
    far, faces, table, ctable, planes, keys, values, first, lines, out_v,
    load_sem, send_sem, recv_sem, out_sem,
):
    count, width = nodes.shape
    held = clusters.shape[0]
    bound = faces.shape[1]
    gx, gy, gz = (lax.axis_index(a) for a in ("gx", "gy", "gz"))
    nx, ny, nz = (lax.axis_size(a) for a in ("gx", "gy", "gz"))
    scale = math.log2(math.e) / math.sqrt(width)

    def along(axis, step):
        at, size = {"gx": (gx, nx), "gy": (gy, ny), "gz": (gz, nz)}[axis]
        return {axis: lax.rem(at + (step % size), size)}

    line = [("gy", s) for s in range(1, ny)]
    line += [("gz", s) for s in range(1, nz)] + [("gx", s) for s in range(1, nx)]
    halo = [(axis, step) for axis in ("gx", "gy", "gz") for step in (1, -1)]

    barrier = pltpu.get_barrier_semaphore()
    for axis, step in line:
        pl.semaphore_signal(barrier, inc=1, device_id=along(axis, step), device_id_type=MESH)

    loads = [
        pltpu.make_async_copy(src, dst, load_sem.at[i])
        for i, (src, dst) in enumerate(
            (
                (nodes_h, nodes), (clusters_h, clusters), (wk_h, wk), (wv_h, wv), (wei_h, wei),
                (weo_h, weo), (wni_h, wni), (wno_h, wno), (gain_h, gain),
            )
        )
    ]
    for copy in loads:
        copy.start()
    loads[0].wait()
    loads[1].wait()
    pl.semaphore_wait(barrier, len(line))

    border = nodes.at[pl.ds(0, bound)]
    sends = []
    for i, (axis, step) in enumerate(halo):
        sends.append(
            pltpu.make_async_remote_copy(
                src_ref=border, dst_ref=faces.at[i], send_sem=send_sem.at[i],
                recv_sem=recv_sem.at[i], device_id=along(axis, step), device_id_type=MESH,
            )
        )
    for i, (axis, step) in enumerate(line):
        j = len(halo) + i
        sends.append(
            pltpu.make_async_remote_copy(
                src_ref=clusters, dst_ref=far.at[i], send_sem=send_sem.at[j],
                recv_sem=recv_sem.at[j], device_id=along(axis, step), device_id_type=MESH,
            )
        )
    for copy in sends:
        copy.start()
    for copy in loads[2:]:
        copy.wait()

    w_kv = jnp.concatenate([wk[...], wv[...]], axis=1)
    values[:, pl.ds(width, width)] = jnp.ones((values.shape[0], width), BF16)

    def project(block, at):
        both = dot(block, w_kv)
        rows = pl.ds(at * held, held)
        keys[rows, :] = both[:, :width].astype(BF16)
        values[rows, pl.ds(0, width)] = both[:, width:].astype(BF16)

    def attend(blocks, before, after):
        reach = pl.ds(0, blocks * held)

        def step(i, carry):
            rows = pl.ds(pl.multiple_of(i * ROWS, ROWS), ROWS)
            scores = lax.dot_general(nodes[rows, :], keys[reach, :], NT, preferred_element_type=F32)
            top = jnp.max(scores, axis=1, keepdims=True)
            if before is None:
                top = jnp.broadcast_to(top, (ROWS, width))
            else:
                old = before[rows, pl.ds(0, width)]
                top = jnp.maximum(old, top)
                fade = jnp.exp2((old - top) * scale)
            weights = jnp.concatenate(
                [
                    jnp.exp2((scores[:, g : g + width] - top) * scale).astype(BF16)
                    for g in range(0, blocks * held, width)
                ],
                axis=1,
            )
            gained = dot(weights, values[reach, :])
            if before is not None:
                gained = gained + before[rows, pl.ds(width, 2 * width)] * jnp.concatenate([fade, fade], axis=1)
            after[rows, pl.ds(0, width)] = top
            after[rows, pl.ds(width, 2 * width)] = gained
            return carry

        lax.fori_loop(0, count // ROWS, step, 0)

    w_sender = wei[pl.ds(width, width), :]
    project(clusters[...], 0)
    attend(1, None, first)
    table[pl.ds(0, count), :] = dot(nodes[...], w_sender)
    ctable[...] = dot(clusters[...], wni[pl.ds(3 * width, width), :])

    at = 0
    for which, size in enumerate((ny, nz, nx)):
        state = lines.at[which]
        before = first
        todo = list(range(at, at + size - 1))
        at += size - 1
        while todo:
            part, todo = (todo, []) if len(todo) <= 3 else (todo[:2], todo[2:])
            for k, i in enumerate(part):
                sends[len(halo) + i].wait_recv()
                project(far[i], k)
            attend(len(part), before, state)
            before = state

    for i in range(len(halo)):
        sends[i].wait_recv()
        table[pl.ds(count + i * bound, bound), :] = dot(faces[i], w_sender)

    degree = senders.shape[0] * senders.shape[1] // count
    unroll = 8

    def pick(i, carry):
        base = pl.multiple_of(i * unroll, unroll)
        per = 128 // degree
        for k in range(unroll):
            for j in range(degree):
                flat = (base + k) * degree + j
                e = senders[lax.div(flat, 128), lax.rem(flat, 128)]
                planes[j, pl.ds(base + k, 1), :] = table[pl.ds(e, 1), :]
            planes[degree, pl.ds(base + k, 1), :] = ctable[pl.ds(members[base + k], 1), :]
        return carry

    lax.fori_loop(0, count // unroll, pick, 0)

    w_out = weo[...]
    w_outs = jnp.concatenate([w_out] * degree, axis=0)
    eps_pool, eps_norm = 1e-06, 1e-05

    def finish(i, carry):
        rows = pl.ds(pl.multiple_of(i * ROWS, ROWS), ROWS)
        own = nodes[rows, :]
        receiver = dot(own, wei[pl.ds(0, width), :])
        hidden = jnp.concatenate([silu(planes[j, rows, :] + receiver).astype(BF16) for j in range(degree)], axis=1)
        aggregated = dot(hidden, w_outs).astype(BF16)
        pooled = jnp.zeros((ROWS, width), F32)
        for which in range(3):
            pooled = pooled + lines[which, rows, pl.ds(width, width)] / lines[which, rows, pl.ds(2 * width, width)]
        attended = (pooled * lax.rsqrt(jnp.mean(pooled * pooled, axis=1, keepdims=True) + eps_pool)).astype(BF16)
        mixed = jnp.concatenate([own, aggregated, attended], axis=1)
        preact = dot(mixed, wni[pl.ds(0, 3 * width), :]) + planes[degree, rows, :]
        update = dot(silu(preact).astype(BF16), wno[...])
        centred = update - jnp.mean(update, axis=1, keepdims=True)
        variance = jnp.mean(centred * centred, axis=1, keepdims=True)
        normed = centred * lax.rsqrt(variance + eps_norm)
        out_v[rows, :] = (own.astype(F32) + normed * gain[...]).astype(BF16)
        return carry

    lax.fori_loop(0, count // ROWS, finish, 0)
    copy = pltpu.make_async_copy(out_v, out_h, out_sem)
    copy.start()
    for sent in sends:
        sent.wait_send()
    copy.wait()


def on_device(mesh, *args):
    nodes, clusters, senders, members, wk, wv, wei, weo, wni, wno, gain = args
    count, width = nodes.shape
    held = clusters.shape[0]
    bound = count // 2
    copies = sum(mesh.shape[a] - 1 for a in ("gx", "gy", "gz"))
    degree = senders.size // count
    hbm = pl.BlockSpec(memory_space=pl.ANY)
    smem = pl.BlockSpec(memory_space=pltpu.SMEM)
    vmem = lambda a: pltpu.VMEM(a.shape, a.dtype)
    gain = gain.reshape(1, width)
    return pl.pallas_call(
        kernel,
        out_shape=jax.ShapeDtypeStruct((count, width), BF16),
        in_specs=[hbm, hbm, smem, smem] + [hbm] * 7,
        out_specs=hbm,
        scratch_shapes=[
            *(vmem(a) for a in (nodes, clusters, wk, wv, wei, weo, wni, wno, gain)),
            pltpu.VMEM((copies, held, width), BF16),
            pltpu.VMEM((6, bound, width), BF16),
            pltpu.VMEM((count + 6 * bound, width), F32),
            pltpu.VMEM((held, width), F32),
            pltpu.VMEM((degree + 1, count, width), F32),
            pltpu.VMEM((3 * held, width), BF16),
            pltpu.VMEM((3 * held, 2 * width), BF16),
            pltpu.VMEM((count, 3 * width), F32),
            pltpu.VMEM((3, count, 3 * width), F32),
            pltpu.VMEM((count, width), BF16),
            pltpu.SemaphoreType.DMA((9,)),
            pltpu.SemaphoreType.DMA((6 + copies,)),
            pltpu.SemaphoreType.DMA((6 + copies,)),
            pltpu.SemaphoreType.DMA,
        ],
        compiler_params=pltpu.CompilerParams(collective_id=0, has_side_effects=True),
        name="layer",
    )(nodes, clusters, senders, members, wk, wv, wei, weo, wni, wno, gain)


def solution(mesh):
    blocks = ("gx", "gy", "gz")
    in_specs = (P(blocks, None), P(blocks, None), P(blocks, None), P(blocks)) + (P(),) * 7
    return jax.shard_map(
        functools.partial(on_device, mesh),
        mesh=mesh, in_specs=in_specs, out_specs=P(blocks, None), check_vma=False,
    )
```

```python
import functools
import math

import jax
import jax.numpy as jnp
from jax import lax
from jax.experimental import pallas as pl
from jax.experimental.pallas import tpu as pltpu
from jax.sharding import PartitionSpec as P

MESH = pl.DeviceIdType.MESH
F32 = jnp.float32
BF16 = jnp.bfloat16
ROWS = 256
BIG = 512
NT = (((1,), (1,)), ((), ()))


def dot(a, b):
    return jnp.dot(a, b, preferred_element_type=F32)


def silu(x):
    half = 0.5 * x
    return half * jnp.tanh(half) + half


def kernel(
    nodes_h, clusters_h, senders_h, members_h, wk_h, wv_h, wei_h, weo_h, wni_h, wno_h, gain_h,
    out_h,
    senders, members, nodes, clusters, wk, wv, wei, weo, wni, wno, gain,
    far, faces, table, ctable, planes, keys, values, first, lines, receiver, base, out_v,
    score_a, score_b, weight_a, weight_b, fade_a, fade_b,
    load_sem, send_sem, recv_sem, out_sem,
):
    count, width = nodes.shape
    held = clusters.shape[0]
    bound = faces.shape[1]
    gx, gy, gz = (lax.axis_index(a) for a in ("gx", "gy", "gz"))
    nx, ny, nz = (lax.axis_size(a) for a in ("gx", "gy", "gz"))
    scale = math.log2(math.e) / math.sqrt(width)

    def along(axis, step):
        at, size = {"gx": (gx, nx), "gy": (gy, ny), "gz": (gz, nz)}[axis]
        return {axis: lax.rem(at + (step % size), size)}

    line = [("gy", s) for s in range(1, ny)]
    line += [("gz", s) for s in (1, nz - 1, 2, nz - 2, 3, nz - 3, 4)]
    line += [("gx", s) for s in (1, nx - 1, 2, nx - 2, 3, nx - 3, 4)]
    halo = [(axis, step) for axis in ("gx", "gy", "gz") for step in (1, -1)]

    barrier = pltpu.get_barrier_semaphore()
    for axis, step in line:
        pl.semaphore_signal(barrier, inc=1, device_id=along(axis, step), device_id_type=MESH)

    loads = [
        pltpu.make_async_copy(src, dst, load_sem.at[i])
        for i, (src, dst) in enumerate(
            (
                (nodes_h, nodes), (clusters_h, clusters), (wk_h, wk), (wv_h, wv), (wei_h, wei),
                (weo_h, weo), (wni_h, wni), (wno_h, wno), (gain_h, gain), (senders_h, senders),
                (members_h, members),
            )
        )
    ]
    for copy in loads:
        copy.start()
    with jax.named_scope("load_wait"):
        loads[0].wait()
        loads[1].wait()
    with jax.named_scope("barrier_wait"):
        pl.semaphore_wait(barrier, len(line))

    border = nodes.at[pl.ds(0, bound)]
    sends = []
    for i, (axis, step) in enumerate(halo):
        sends.append(
            pltpu.make_async_remote_copy(
                src_ref=border, dst_ref=faces.at[i], send_sem=send_sem.at[i],
                recv_sem=recv_sem.at[i], device_id=along(axis, step), device_id_type=MESH,
            )
        )
    for i, (axis, step) in enumerate(line):
        j = len(halo) + i
        sends.append(
            pltpu.make_async_remote_copy(
                src_ref=clusters, dst_ref=far.at[i], send_sem=send_sem.at[j],
                recv_sem=recv_sem.at[j], device_id=along(axis, step), device_id_type=MESH,
            )
        )
    for copy in sends:
        copy.start()
    for copy in loads[2:]:
        copy.wait()

    w_kv = jnp.concatenate([wk[...], wv[...]], axis=1)
    values[:, pl.ds(width, width)] = jnp.ones((values.shape[0], width), BF16)

    def project(block, at):
        both = dot(block, w_kv)
        rows = pl.ds(at * held, held)
        keys[rows, :] = both[:, :width].astype(BF16)
        values[rows, pl.ds(0, width)] = both[:, width:].astype(BF16)

    steps = count // ROWS
    score, weight, fades = (score_a, score_b), (weight_a, weight_b), (fade_a, fade_b)

    def attend(at, blocks, before, after):
        span = blocks * held
        reach, near = pl.ds(at * held, span), pl.ds(0, span)

        def rows_of(i):
            return pl.ds(i * ROWS if isinstance(i, int) else pl.multiple_of(i * ROWS, ROWS), ROWS)

        def scores_of(i, p):
            score[p][:, near] = lax.dot_general(nodes[rows_of(i), :], keys[reach, :], NT, preferred_element_type=F32)

        def weights_of(i, p):
            rows = rows_of(i)
            scores = score[p][:, near]
            top = jnp.max(scores, axis=1, keepdims=True)
            if before is None:
                top = jnp.broadcast_to(top, (ROWS, width))
            else:
                old = before[rows, pl.ds(0, width)]
                top = jnp.maximum(old, top)
                fades[p][...] = jnp.exp2((old - top) * scale)
            after[rows, pl.ds(0, width)] = top
            for g in range(0, span, width):
                weight[p][:, pl.ds(g, width)] = jnp.exp2((scores[:, g : g + width] - top) * scale).astype(BF16)

        def sums_of(i, p):
            rows, both = rows_of(i), pl.ds(width, 2 * width)
            gained = dot(weight[p][:, near], values[reach, :])
            if before is not None:
                fade = fades[p][...]
                gained = gained + before[rows, both] * jnp.concatenate([fade, fade], axis=1)
            after[rows, both] = gained

        scores_of(0, 0)
        scores_of(1, 1)
        weights_of(0, 0)

        def step(j, carry):
            for p in range(2):
                sums_of(2 * j + p, p)
                weights_of(2 * j + p + 1, 1 - p)
                scores_of(2 * j + p + 2, p)
            return carry

        with jax.named_scope(f"attend{blocks}"):
            lax.fori_loop(0, steps // 2 - 1, step, 0)
        sums_of(steps - 2, 0)
        weights_of(steps - 1, 1)
        sums_of(steps - 1, 1)

    own_w, sender_w = pl.ds(0, width), pl.ds(width, width)
    project(clusters[...], 0)
    attend(0, 1, None, first)
    table[pl.ds(0, count), :] = dot(nodes[...], wei[sender_w, :])
    receiver[...] = dot(nodes[...], wei[own_w, :])
    ctable[...] = dot(clusters[...], wni[pl.ds(3 * width, width), :])

    for i in range(len(halo)):
        with jax.named_scope(f"wait_halo{i}"):
            sends[i].wait_recv()
        table[pl.ds(count + i * bound, bound), :] = dot(faces[i], wei[sender_w, :])

    degree = senders.shape[0] * senders.shape[1] // count
    lanes = senders.shape[1]
    part = lanes // degree

    def pick(i, carry):
        start = pl.multiple_of(i * part, part)
        for k in range(part):
            for j in range(degree):
                planes[j, pl.ds(start + k, 1), :] = table[pl.ds(senders[i, k * degree + j], 1), :]
            planes[degree, pl.ds(start + k, 1), :] = ctable[pl.ds(members[start + k], 1), :]
        return carry

    with jax.named_scope("gather"):
        lax.fori_loop(0, senders.shape[0], pick, 0)

    w_out = weo[...]
    w_outs = jnp.concatenate([w_out] * degree, axis=0)

    def edges(i, carry):
        rows = pl.ds(pl.multiple_of(i * BIG, BIG), BIG)
        to = receiver[rows, :]
        hidden = jnp.concatenate([silu(planes[j, rows, :] + to).astype(BF16) for j in range(degree)], axis=1)
        aggregated = dot(hidden, w_outs).astype(BF16)
        mixed = jnp.concatenate([nodes[rows, :], aggregated], axis=1)
        base[rows, :] = dot(mixed, wni[pl.ds(0, 2 * width), :]) + planes[degree, rows, :]
        return carry

    with jax.named_scope("edges"):
        lax.fori_loop(0, count // BIG, edges, 0)

    at = 0
    for which, size in enumerate((ny, nz, nx)):
        state = lines.at[which]
        before = first
        todo = list(range(at, at + size - 1))
        at += size - 1
        while todo:
            now = min(len(todo), 3 if len(todo) != 4 else 4)
            now, todo = todo[:now], todo[now:]
            for i in now:
                with jax.named_scope(f"wait_line{i}"):
                    sends[len(halo) + i].wait_recv()
                project(far[i], i + 1)
            attend(now[0] + 1, len(now), before, state)
            before = state

    eps_pool, eps_norm = 1e-06, 1e-05

    def finish(i, carry):
        rows = pl.ds(pl.multiple_of(i * BIG, BIG), BIG)
        pooled = jnp.zeros((BIG, width), F32)
        for which in range(3):
            pooled = pooled + lines[which, rows, pl.ds(width, width)] / lines[which, rows, pl.ds(2 * width, width)]
        attended = (pooled * lax.rsqrt(jnp.mean(pooled * pooled, axis=1, keepdims=True) + eps_pool)).astype(BF16)
        preact = dot(attended, wni[pl.ds(2 * width, width), :]) + base[rows, :]
        update = dot(silu(preact).astype(BF16), wno[...])
        centred = update - jnp.mean(update, axis=1, keepdims=True)
        variance = jnp.mean(centred * centred, axis=1, keepdims=True)
        normed = centred * lax.rsqrt(variance + eps_norm)
        out_v[rows, :] = (nodes[rows, :].astype(F32) + normed * gain[...]).astype(BF16)
        return carry

    with jax.named_scope("finish"):
        lax.fori_loop(0, count // BIG, finish, 0)
    copy = pltpu.make_async_copy(out_v, out_h, out_sem)
    copy.start()
    with jax.named_scope("end"):
        for sent in sends:
            sent.wait_send()
        copy.wait()


def on_device(mesh, *args):
    nodes, clusters, senders, members, wk, wv, wei, weo, wni, wno, gain = args
    count, width = nodes.shape
    held = clusters.shape[0]
    bound = count // 2
    copies = sum(mesh.shape[a] - 1 for a in ("gx", "gy", "gz"))
    degree = senders.size // count
    hbm = pl.BlockSpec(memory_space=pl.ANY)
    vmem = lambda a: pltpu.VMEM(a.shape, a.dtype)
    gain = gain.reshape(1, width)
    return pl.pallas_call(
        kernel,
        out_shape=jax.ShapeDtypeStruct((count, width), BF16),
        in_specs=[hbm] * 11,
        out_specs=hbm,
        scratch_shapes=[
            pltpu.SMEM(senders.shape, senders.dtype),
            pltpu.SMEM(members.shape, members.dtype),
            *(vmem(a) for a in (nodes, clusters, wk, wv, wei, weo, wni, wno, gain)),
            pltpu.VMEM((copies, held, width), BF16),
            pltpu.VMEM((6, bound, width), BF16),
            pltpu.VMEM((count + 6 * bound, width), F32),
            pltpu.VMEM((held, width), F32),
            pltpu.VMEM((degree + 1, count, width), F32),
            pltpu.VMEM(((copies + 1) * held, width), BF16),
            pltpu.VMEM(((copies + 1) * held, 2 * width), BF16),
            pltpu.VMEM((count, 3 * width), F32),
            pltpu.VMEM((3, count, 3 * width), F32),
            pltpu.VMEM((count, width), F32),
            pltpu.VMEM((count, width), F32),
            pltpu.VMEM((count, width), BF16),
            *[pltpu.VMEM((ROWS, 4 * held), F32)] * 2,
            *[pltpu.VMEM((ROWS, 4 * held), BF16)] * 2,
            *[pltpu.VMEM((ROWS, width), F32)] * 2,
            pltpu.SemaphoreType.DMA((11,)),
            pltpu.SemaphoreType.DMA((6 + copies,)),
            pltpu.SemaphoreType.DMA((6 + copies,)),
            pltpu.SemaphoreType.DMA,
        ],
        compiler_params=pltpu.CompilerParams(collective_id=0, has_side_effects=True),
        name="layer",
    )(nodes, clusters, senders, members, wk, wv, wei, weo, wni, wno, gain)


def solution(mesh):
    blocks = ("gx", "gy", "gz")
    in_specs = (P(blocks, None), P(blocks, None), P(blocks, None), P(blocks)) + (P(),) * 7
    return jax.shard_map(
        functools.partial(on_device, mesh),
        mesh=mesh, in_specs=in_specs, out_specs=P(blocks, None), check_vma=False,
    )
```

```python
import functools
import math

import jax
import jax.numpy as jnp
from jax import lax
from jax.experimental import pallas as pl
from jax.experimental.pallas import tpu as pltpu
from jax.sharding import PartitionSpec as P

MESH = pl.DeviceIdType.MESH
F32 = jnp.float32
BF16 = jnp.bfloat16
ROWS = 256
BIG = 512
NT = (((1,), (1,)), ((), ()))


def dot(a, b):
    return jnp.dot(a, b, preferred_element_type=F32)


def silu(x):
    half = 0.5 * x
    return half * jnp.tanh(half) + half


def kernel(
    nodes_h, clusters_h, senders_h, members_h, wk_h, wv_h, wei_h, weo_h, wni_h, wno_h, gain_h,
    out_h,
    senders, members, nodes, clusters, wk, wv, wei, weo, wni, wno, gain,
    far, faces, table, ctable, planes, keys, values, first, lines, receiver, base, out_v,
    score_a, score_b, weight_a, weight_b, fade_a, fade_b,
    load_sem, send_sem, recv_sem, out_sem,
):
    count, width = nodes.shape
    held = clusters.shape[0]
    bound = faces.shape[0] // 6
    gx, gy, gz = (lax.axis_index(a) for a in ("gx", "gy", "gz"))
    nx, ny, nz = (lax.axis_size(a) for a in ("gx", "gy", "gz"))
    scale = math.log2(math.e) / math.sqrt(width)

    half = ny_ring = nx // 2
    upper, ring = lax.div(gx, ny_ring), lax.rem(gx, ny_ring)

    def to_gy(d):
        return {"gy": lax.rem(gy + d % ny, ny)}

    def to_gz(d):
        return {"gz": lax.rem(gz + d % nz, nz)}

    def to_gx(d):
        return {"gx": lax.rem(gx + d % nx, nx)}

    def to_ring(d):
        return {"gx": upper * ny_ring + lax.rem(ring + d % ny_ring, ny_ring)}

    across = {"gx": lax.rem(gx + half, nx)}
    halo = [to_gx(1), to_gx(-1), to_gy(1), to_gy(-1), to_gz(1), to_gz(-1)]
    partners = [to_gy(d) for d in (1, 2, 3)] + [to_gz(d) for d in (1, -1, 2, -2)]
    partners += [across] + [to_ring(d) for d in (1, -1, 2)] + [to_gx(1), to_gx(-1)]

    barrier = pltpu.get_barrier_semaphore()
    for device in partners:
        pl.semaphore_signal(barrier, inc=1, device_id=device, device_id_type=MESH)

    loads = [
        pltpu.make_async_copy(src, dst, load_sem.at[i])
        for i, (src, dst) in enumerate(
            (
                (nodes_h, nodes), (clusters_h, clusters), (wk_h, wk), (wv_h, wv), (wei_h, wei),
                (weo_h, weo), (wni_h, wni), (wno_h, wno), (gain_h, gain), (senders_h, senders),
                (members_h, members),
            )
        )
    ]
    for copy in loads:
        copy.start()
    with jax.named_scope("load_wait"):
        loads[0].wait()
        loads[1].wait()
    with jax.named_scope("barrier_wait"):
        pl.semaphore_wait(barrier, len(partners))

    slots = ["y1", "y2", "y3", "z-1", "z1", "z-2", "z2", "z-3", "z3", "z4"]
    slots += ["x", "r-1", "r1", "r2", "xr-1", "xr1", "xr2"]
    slot = {name: i for i, name in enumerate(slots)}
    copies = {}

    def send(key, src, dst, device):
        i = len(copies)
        copies[key] = pltpu.make_async_remote_copy(
            src_ref=src, dst_ref=dst, send_sem=send_sem.at[i], recv_sem=recv_sem.at[i],
            device_id=device, device_id_type=MESH,
        )
        copies[key].start()

    def cell(name, start=0, size=held):
        return far.at[pl.ds(slot[name] * held + start, size)]

    send("x", clusters, cell("x"), across)
    send("z-2", clusters, cell("z-2"), to_gz(2))
    send("z2", clusters, cell("z2"), to_gz(-2))
    for d in (1, 2, 3):
        send(f"y{d}", clusters, cell(f"y{d}"), to_gy(-d))
    send("z-1", clusters, cell("z-1"), to_gz(1))
    send("z1", clusters, cell("z1"), to_gz(-1))
    send("r-1", clusters, cell("r-1"), to_ring(1))
    send("r1", clusters, cell("r1"), to_ring(-1))
    border = nodes.at[pl.ds(0, bound)]
    for i, device in enumerate(halo):
        send(f"h{i}", border, faces.at[pl.ds(i * bound, bound)], device)
    send("r2", clusters, cell("r2"), to_ring(2))

    def arrive(*names):
        for name in names:
            with jax.named_scope("wait_" + name):
                copies[name].wait_recv()

    def relay_x():
        arrive("x")
        for d in (1, -1, 2):
            name = "xr2" if d == 2 else f"xr{-d}"
            send(name, cell("x"), cell(name), to_ring(d))

    def relay_z():
        for sign, start in ((-1, 0), (1, held // 2)):
            here = f"z{2 * sign}"
            arrive(here)
            send(f"z{3 * sign}", cell(here), cell(f"z{3 * sign}"), to_gz(-sign))
            send(f"z4_{start}", cell(here, start, held // 2), cell("z4", start, held // 2), to_gz(-2 * sign))

    for copy in loads[2:]:
        copy.wait()

    w_kv = jnp.concatenate([wk[...], wv[...]], axis=1)
    values[:, pl.ds(width, width)] = jnp.ones((values.shape[0], width), BF16)

    def project(block, at, blocks):
        both = dot(block, w_kv)
        rows = pl.ds(at * held, blocks * held)
        keys[rows, :] = both[:, :width].astype(BF16)
        values[rows, pl.ds(0, width)] = both[:, width:].astype(BF16)

    steps = count // ROWS
    score, weight, fades = (score_a, score_b), (weight_a, weight_b), (fade_a, fade_b)

    def rows_of(i):
        return pl.ds(i * ROWS, ROWS)

    def scores_of(at, blocks, before, after, i, p):
        reach, near = pl.ds(at * held, blocks * held), pl.ds(0, blocks * held)
        score[p][:, near] = lax.dot_general(nodes[rows_of(i), :], keys[reach, :], NT, preferred_element_type=F32)

    def weights_of(at, blocks, before, after, i, p):
        span = blocks * held
        rows = rows_of(i)
        scores = score[p][:, pl.ds(0, span)]
        top = jnp.max(scores, axis=1, keepdims=True)
        if before is None:
            top = jnp.broadcast_to(top, (ROWS, width))
        else:
            old = before[rows, pl.ds(0, width)]
            top = jnp.maximum(old, top)
            fades[p][...] = jnp.exp2((old - top) * scale)
        after[rows, pl.ds(0, width)] = top
        for g in range(0, span, width):
            weight[p][:, pl.ds(g, width)] = jnp.exp2((scores[:, g : g + width] - top) * scale).astype(BF16)

    def sums_of(at, blocks, before, after, i, p):
        reach, near = pl.ds(at * held, blocks * held), pl.ds(0, blocks * held)
        rows, both = rows_of(i), pl.ds(width, 2 * width)
        gained = dot(weight[p][:, near], values[reach, :])
        if before is not None:
            fade = fades[p][...]
            gained = gained + before[rows, both] * jnp.concatenate([fade, fade], axis=1)
        after[rows, both] = gained

    line = []

    def advance(entry):
        n = len(line)
        if n >= 2 and line[n - 2]:
            sums_of(*line[n - 2], n % 2)
        if n >= 1 and line[n - 1]:
            weights_of(*line[n - 1], (n - 1) % 2)
        line.append(entry)
        if entry:
            scores_of(*entry, n % 2)

    def attend(names, before, after):
        first_slot = slot[names[0]] + 1 if names else 0
        blocks = max(len(names), 1)
        if names:
            project(far[pl.ds((first_slot - 1) * held, blocks * held), :], first_slot, blocks)
        else:
            project(clusters[...], 0, 1)
        for i in range(steps):
            advance((first_slot, blocks, before, after, i))

    own_w, sender_w = pl.ds(0, width), pl.ds(width, width)
    attend((), None, first)
    table[pl.ds(0, count), :] = dot(nodes[...], wei[sender_w, :])
    receiver[...] = dot(nodes[...], wei[own_w, :])
    ctable[...] = dot(clusters[...], wni[pl.ds(3 * width, width), :])
    relay_x()
    arrive("y1", "y2", "y3")
    attend(("y1", "y2", "y3"), first, lines.at[0])
    relay_z()
    arrive("z-1", "z1")
    attend(("z-1", "z1", "z-2", "z2"), first, lines.at[1])
    for i in range(len(halo)):
        arrive(f"h{i}")
    table[pl.ds(count, 6 * bound), :] = dot(faces[...], wei[sender_w, :])

    degree = senders.shape[0] * senders.shape[1] // count
    lanes = senders.shape[1]
    part = lanes // degree

    def pick(i, carry):
        start = pl.multiple_of(i * part, part)
        for k in range(part):
            for j in range(degree):
                planes[j, pl.ds(start + k, 1), :] = table[pl.ds(senders[i, k * degree + j], 1), :]
            planes[degree, pl.ds(start + k, 1), :] = ctable[pl.ds(members[start + k], 1), :]
        return carry

    with jax.named_scope("gather"):
        lax.fori_loop(0, senders.shape[0], pick, 0)

    w_out = weo[...]
    w_outs = jnp.concatenate([w_out] * degree, axis=0)

    def edges(i, carry):
        rows = pl.ds(pl.multiple_of(i * BIG, BIG), BIG)
        to = receiver[rows, :]
        hidden = jnp.concatenate([silu(planes[j, rows, :] + to).astype(BF16) for j in range(degree)], axis=1)
        aggregated = dot(hidden, w_outs).astype(BF16)
        mixed = jnp.concatenate([nodes[rows, :], aggregated], axis=1)
        base[rows, :] = dot(mixed, wni[pl.ds(0, 2 * width), :]) + planes[degree, rows, :]
        return carry

    with jax.named_scope("edges"):
        lax.fori_loop(0, count // BIG, edges, 0)

    arrive("r-1", "r1", "r2")
    attend(("x", "r-1", "r1", "r2"), first, lines.at[2])
    arrive("xr-1", "xr1", "xr2")
    attend(("xr-1", "xr1", "xr2"), lines.at[2], lines.at[2])
    arrive("z-3", "z3", "z4_0", f"z4_{held // 2}")
    attend(("z-3", "z3", "z4"), lines.at[1], lines.at[1])
    advance(None)
    advance(None)

    eps_pool, eps_norm = 1e-06, 1e-05

    def finish(i, carry):
        rows = pl.ds(pl.multiple_of(i * BIG, BIG), BIG)
        pooled = jnp.zeros((BIG, width), F32)
        for which in range(3):
            pooled = pooled + lines[which, rows, pl.ds(width, width)] / lines[which, rows, pl.ds(2 * width, width)]
        attended = (pooled * lax.rsqrt(jnp.mean(pooled * pooled, axis=1, keepdims=True) + eps_pool)).astype(BF16)
        preact = dot(attended, wni[pl.ds(2 * width, width), :]) + base[rows, :]
        update = dot(silu(preact).astype(BF16), wno[...])
        centred = update - jnp.mean(update, axis=1, keepdims=True)
        variance = jnp.mean(centred * centred, axis=1, keepdims=True)
        normed = centred * lax.rsqrt(variance + eps_norm)
        out_v[rows, :] = (nodes[rows, :].astype(F32) + normed * gain[...]).astype(BF16)
        return carry

    with jax.named_scope("finish"):
        lax.fori_loop(0, count // BIG, finish, 0)
    copy = pltpu.make_async_copy(out_v, out_h, out_sem)
    copy.start()
    with jax.named_scope("end"):
        for sent in copies.values():
            sent.wait_send()
        copy.wait()


def on_device(mesh, *args):
    nodes, clusters, senders, members, wk, wv, wei, weo, wni, wno, gain = args
    count, width = nodes.shape
    held = clusters.shape[0]
    bound = count // 2
    copies = sum(mesh.shape[a] - 1 for a in ("gx", "gy", "gz"))
    degree = senders.size // count
    hbm = pl.BlockSpec(memory_space=pl.ANY)
    vmem = lambda a: pltpu.VMEM(a.shape, a.dtype)
    gain = gain.reshape(1, width)
    return pl.pallas_call(
        kernel,
        out_shape=jax.ShapeDtypeStruct((count, width), BF16),
        in_specs=[hbm] * 11,
        out_specs=hbm,
        scratch_shapes=[
            pltpu.SMEM(senders.shape, senders.dtype),
            pltpu.SMEM(members.shape, members.dtype),
            *(vmem(a) for a in (nodes, clusters, wk, wv, wei, weo, wni, wno, gain)),
            pltpu.VMEM((copies * held, width), BF16),
            pltpu.VMEM((6 * bound, width), BF16),
            pltpu.VMEM((count + 6 * bound, width), F32),
            pltpu.VMEM((held, width), F32),
            pltpu.VMEM((degree + 1, count, width), F32),
            pltpu.VMEM(((copies + 1) * held, width), BF16),
            pltpu.VMEM(((copies + 1) * held, 2 * width), BF16),
            pltpu.VMEM((count, 3 * width), F32),
            pltpu.VMEM((3, count, 3 * width), F32),
            pltpu.VMEM((count, width), F32),
            pltpu.VMEM((count, width), F32),
            pltpu.VMEM((count, width), BF16),
            *[pltpu.VMEM((ROWS, 4 * held), F32)] * 2,
            *[pltpu.VMEM((ROWS, 4 * held), BF16)] * 2,
            *[pltpu.VMEM((ROWS, width), F32)] * 2,
            pltpu.SemaphoreType.DMA((11,)),
            pltpu.SemaphoreType.DMA((7 + copies,)),
            pltpu.SemaphoreType.DMA((7 + copies,)),
            pltpu.SemaphoreType.DMA,
        ],
        compiler_params=pltpu.CompilerParams(collective_id=0, has_side_effects=True),
        name="layer",
    )(nodes, clusters, senders, members, wk, wv, wei, weo, wni, wno, gain)


def solution(mesh):
    blocks = ("gx", "gy", "gz")
    in_specs = (P(blocks, None), P(blocks, None), P(blocks, None), P(blocks)) + (P(),) * 7
    return jax.shard_map(
        functools.partial(on_device, mesh),
        mesh=mesh, in_specs=in_specs, out_specs=P(blocks, None), check_vma=False,
    )
```

```python
import functools
import math

import jax
import jax.numpy as jnp
from jax import lax
from jax.experimental import pallas as pl
from jax.experimental.pallas import tpu as pltpu
from jax.sharding import PartitionSpec as P

MESH = pl.DeviceIdType.MESH
F32 = jnp.float32
BF16 = jnp.bfloat16
ROWS = 256
BIG = 512
PAD = 8
NT = (((1,), (1,)), ((), ()))


def dot(a, b):
    return jnp.dot(a, b, preferred_element_type=F32)


def silu(x):
    half = 0.5 * x
    return half * jnp.tanh(half) + half


def kernel(
    nodes_h, clusters_h, senders_h, members_h, wk_h, wv_h, wei_h, weo_h, wni_h, wno_h, gain_h,
    out_h,
    senders, members, nodes, clusters, wk, wv, wei, weo, wni, wno, gain,
    far, faces, table, ctable, planes, keys, values, first, lines, receiver, base, out_v,
    score_a, score_b,
    load_sem, send_sem, recv_sem, out_sem,
):
    count, width = nodes.shape
    held = clusters.shape[0]
    bound = faces.shape[0] // 6
    gx, gy, gz = (lax.axis_index(a) for a in ("gx", "gy", "gz"))
    nx, ny, nz = (lax.axis_size(a) for a in ("gx", "gy", "gz"))
    scale = math.log2(math.e) / math.sqrt(width)

    half = ny_ring = nx // 2
    upper, ring = lax.div(gx, ny_ring), lax.rem(gx, ny_ring)

    core = gy + 1 - 2 * lax.rem(gy, 2)
    side = lax.rem(gy + ny // 2, ny)
    diagonal = lax.rem(core + ny // 2, ny)
    to_gy = {"core": {"gy": core}, "side": {"gy": side}, "diag": {"gy": diagonal}}

    def to_gz(d):
        return {"gz": lax.rem(gz + d % nz, nz)}

    def to_gx(d):
        return {"gx": lax.rem(gx + d % nx, nx)}

    def to_ring(d):
        return {"gx": upper * ny_ring + lax.rem(ring + d % ny_ring, ny_ring)}

    across = {"gx": lax.rem(gx + half, nx)}
    halo = [to_gx(1), to_gx(-1), {"gy": lax.rem(gy + 1, ny)}, {"gy": lax.rem(gy + ny - 1, ny)}, to_gz(1), to_gz(-1)]
    partners = [*to_gy.values()] + [to_gz(d) for d in (1, -1, 2, -2)]
    partners += [across] + [to_ring(d) for d in (1, -1, 2)] + [to_gx(1), to_gx(-1)]

    barrier = pltpu.get_barrier_semaphore()
    for device in partners:
        pl.semaphore_signal(barrier, inc=1, device_id=device, device_id_type=MESH)

    loads = [
        pltpu.make_async_copy(src, dst, load_sem.at[i])
        for i, (src, dst) in enumerate(
            (
                (nodes_h, nodes), (clusters_h, clusters), (wk_h, wk), (wv_h, wv), (wei_h, wei),
                (weo_h, weo), (wni_h, wni), (wno_h, wno), (gain_h, gain), (senders_h, senders),
                (members_h, members),
            )
        )
    ]
    for copy in loads:
        copy.start()
    with jax.named_scope("load_wait"):
        loads[0].wait()
        loads[1].wait()
    with jax.named_scope("barrier_wait"):
        pl.semaphore_wait(barrier, len(partners))

    slots = ["core", "side", "diag", "z-1", "z1", "z-2", "z2", "z-3", "z3", "z4"]
    slots += ["r-1", "r1", "x", "r2", "xr-1", "xr1", "xr2"]
    slot = {name: i for i, name in enumerate(slots)}
    copies = {}

    def send(key, src, dst, device):
        i = len(copies)
        copies[key] = pltpu.make_async_remote_copy(
            src_ref=src, dst_ref=dst, send_sem=send_sem.at[i], recv_sem=recv_sem.at[i],
            device_id=device, device_id_type=MESH,
        )
        copies[key].start()

    def cell(name, start=0, size=held):
        return far.at[pl.ds(slot[name] * held + start, size)]

    send("core", clusters, cell("core"), to_gy["core"])
    send("x", clusters, cell("x"), across)
    send("z-1", clusters, cell("z-1"), to_gz(1))
    send("z1", clusters, cell("z1"), to_gz(-1))
    send("r-1", clusters, cell("r-1"), to_ring(1))
    send("r1", clusters, cell("r1"), to_ring(-1))
    send("side", clusters, cell("side"), to_gy["side"])
    send("diag", clusters, cell("diag"), to_gy["diag"])
    border = nodes.at[pl.ds(0, bound)]
    for i, device in enumerate(halo):
        send(f"h{i}", border, faces.at[pl.ds(i * bound, bound)], device)
    send("z-2", clusters, cell("z-2"), to_gz(2))
    send("z2", clusters, cell("z2"), to_gz(-2))
    send("r2", clusters, cell("r2"), to_ring(2))

    def arrive(*names):
        for name in names:
            with jax.named_scope("wait_" + name):
                copies[name].wait_recv()

    def relay_x():
        arrive("x")
        for d in (1, -1, 2):
            name = "xr2" if d == 2 else f"xr{-d}"
            send(name, cell("x"), cell(name), to_ring(d))

    def relay_z():
        for sign, start in ((-1, 0), (1, held // 2)):
            here = f"z{2 * sign}"
            arrive(here)
            send(f"z{3 * sign}", cell(here), cell(f"z{3 * sign}"), to_gz(-sign))
            send(f"z4_{start}", cell(here, start, held // 2), cell("z4", start, held // 2), to_gz(-2 * sign))

    for copy in loads[2:]:
        copy.wait()

    w_kv = jnp.concatenate([wk[...], wv[...]], axis=1)
    values[:, pl.ds(width, width)] = jnp.ones((values.shape[0], width), F32)

    def project(block, at, blocks):
        both = dot(block, w_kv)
        rows = pl.ds(at * held, blocks * held)
        keys[rows, :] = both[:, :width].astype(BF16)
        values[rows, pl.ds(0, width)] = both[:, width:].astype(BF16).astype(F32)

    steps = count // ROWS
    score = (score_a, score_b)

    def rows_of(i):
        return pl.ds(i * ROWS, ROWS)

    def scores_of(at, blocks, before, after, i, p):
        reach, near = pl.ds(at * held, blocks * held), pl.ds(0, blocks * held)
        score[p][:, near] = lax.dot_general(nodes[rows_of(i), :], keys[reach, :], NT, preferred_element_type=F32)

    def sums_of(at, blocks, before, after, i, p):
        span = blocks * held
        rows, both = rows_of(i), pl.ds(width, 2 * width)
        scores = score[p][:, pl.ds(0, span)]
        top = jnp.max(scores, axis=1, keepdims=True)
        if before is None:
            top = jnp.broadcast_to(top, (ROWS, width))
        else:
            old = before[rows, pl.ds(0, width)]
            top = jnp.maximum(old, top)
            fade = jnp.exp2((old - top) * scale)
        after[rows, pl.ds(0, width)] = top
        weight = [jnp.exp2((scores[:, g : g + width] - top) * scale) for g in range(0, span, width)]
        gained = dot(jnp.concatenate(weight, axis=1), values[pl.ds(at * held, span), :])
        if before is not None:
            gained = gained + before[rows, both] * jnp.concatenate([fade, fade], axis=1)
        after[rows, both] = gained

    line = []

    def advance(entry):
        n = len(line)
        line.append(entry)
        if entry:
            scores_of(*entry, n % 2)
        if n >= 1:
            sums_of(*line[n - 1], (n - 1) % 2)

    def attend(names, before, after, fill=None):
        first_slot = slot[names[0]] + 1 if names else 0
        blocks = max(len(names), 1)
        if names:
            project(far[pl.ds((first_slot - 1) * held, blocks * held), :], first_slot, blocks)
        else:
            project(clusters[...], 0, 1)
        for i in range(steps):
            advance((first_slot, blocks, before, after, i))
            if fill is not None:
                fill(i)

    own_w, sender_w = pl.ds(0, width), pl.ds(width, width)
    attend((), None, first)
    table[pl.ds(PAD, count), :] = dot(nodes[...], wei[sender_w, :])
    receiver[...] = dot(nodes[...], wei[own_w, :])
    for padded in (table, ctable):
        padded[pl.ds(0, PAD), :] = jnp.zeros((PAD, width), F32)
        padded[pl.ds(padded.shape[0] - PAD, PAD), :] = jnp.zeros((PAD, width), F32)
    ctable[pl.ds(PAD, held), :] = dot(clusters[...], wni[pl.ds(3 * width, width), :])
    arrive("core")
    attend(("core",), first, lines.at[0])
    arrive("z-1", "z1")
    attend(("z-1", "z1"), first, lines.at[1])
    relay_x()
    arrive("r-1", "r1")
    attend(("r-1", "r1"), first, lines.at[2])
    arrive("side", "diag")
    attend(("side", "diag"), lines.at[0], lines.at[0])

    degree = senders.shape[0] * senders.shape[1] // count
    lanes = senders.shape[1]
    part = lanes // degree

    sublane = lax.broadcasted_iota(jnp.int32, (PAD, width), 0)

    def pick_rows(source, places):
        rows = None
        for k, place in enumerate(places):
            loaded = source[pl.ds(place + (PAD - k), PAD), :]
            rows = loaded if rows is None else jnp.where(sublane == k, loaded, rows)
        return rows

    def pick(i):
        for start in range(i * part, i * part + part, PAD):
            ends = range(start, start + PAD)
            for j in range(degree):
                flat = [n * degree + j for n in ends]
                planes[j, pl.ds(start, PAD), :] = pick_rows(table, [senders[f // lanes, f % lanes] for f in flat])
            planes[degree, pl.ds(start, PAD), :] = pick_rows(ctable, [members[n] for n in ends])

    def picks(begin, each):
        def fill(i):
            for m in range(begin + i * each, begin + i * each + each):
                pick(m)

        return fill

    w_out = weo[...]
    w_outs = jnp.concatenate([w_out] * degree, axis=0)

    def edges(i):
        rows = rows_of(i)
        to = receiver[rows, :]
        hidden = jnp.concatenate([silu(planes[j, rows, :] + to).astype(BF16) for j in range(degree)], axis=1)
        aggregated = dot(hidden, w_outs).astype(BF16)
        mixed = jnp.concatenate([nodes[rows, :], aggregated], axis=1)
        base[rows, :] = dot(mixed, wni[pl.ds(0, 2 * width), :]) + planes[degree, rows, :]

    for i in range(len(halo)):
        arrive(f"h{i}")
    table[pl.ds(PAD + count, 6 * bound), :] = dot(faces[...], wei[sender_w, :])
    each = senders.shape[0] // (2 * steps)
    relay_z()
    arrive("r2")
    attend(("x", "r2"), lines.at[2], lines.at[2], picks(0, each))
    arrive("xr-1", "xr1", "xr2")
    attend(("xr-1", "xr1", "xr2"), lines.at[2], lines.at[2], picks(steps * each, each))
    attend(("z-2", "z2"), lines.at[1], lines.at[1], edges)
    arrive("z-3", "z3", "z4_0", f"z4_{held // 2}")
    attend(("z-3", "z3", "z4"), lines.at[1], lines.at[1])
    advance(None)

    eps_pool, eps_norm = 1e-06, 1e-05

    def finish(i, carry):
        rows = pl.ds(i * BIG, BIG)
        pooled = jnp.zeros((BIG, width), F32)
        for which in range(3):
            pooled = pooled + lines[which, rows, pl.ds(width, width)] / lines[which, rows, pl.ds(2 * width, width)]
        attended = (pooled * lax.rsqrt(jnp.mean(pooled * pooled, axis=1, keepdims=True) + eps_pool)).astype(BF16)
        preact = dot(attended, wni[pl.ds(2 * width, width), :]) + base[rows, :]
        update = dot(silu(preact).astype(BF16), wno[...])
        centred = update - jnp.mean(update, axis=1, keepdims=True)
        variance = jnp.mean(centred * centred, axis=1, keepdims=True)
        normed = centred * lax.rsqrt(variance + eps_norm)
        out_v[rows, :] = (nodes[rows, :].astype(F32) + normed * gain[...]).astype(BF16)
        return carry

    pieces = []
    with jax.named_scope("finish"):
        for i in range(count // BIG):
            finish(i, 0)
            rows = pl.ds(i * BIG, BIG)
            pieces.append(pltpu.make_async_copy(out_v.at[rows], out_h.at[rows], out_sem.at[i]))
            pieces[-1].start()
    with jax.named_scope("end"):
        for sent in copies.values():
            sent.wait_send()
        for copy in pieces:
            copy.wait()


def on_device(mesh, *args):
    nodes, clusters, senders, members, wk, wv, wei, weo, wni, wno, gain = args
    count, width = nodes.shape
    held = clusters.shape[0]
    bound = count // 2
    copies = sum(mesh.shape[a] - 1 for a in ("gx", "gy", "gz"))
    degree = senders.size // count
    hbm = pl.BlockSpec(memory_space=pl.ANY)
    vmem = lambda a: pltpu.VMEM(a.shape, a.dtype)
    gain = gain.reshape(1, width)
    return pl.pallas_call(
        kernel,
        out_shape=jax.ShapeDtypeStruct((count, width), BF16),
        in_specs=[hbm] * 11,
        out_specs=hbm,
        scratch_shapes=[
            pltpu.SMEM(senders.shape, senders.dtype),
            pltpu.SMEM(members.shape, members.dtype),
            *(vmem(a) for a in (nodes, clusters, wk, wv, wei, weo, wni, wno, gain)),
            pltpu.VMEM((copies * held, width), BF16),
            pltpu.VMEM((6 * bound, width), BF16),
            pltpu.VMEM((count + 6 * bound + 2 * PAD, width), F32),
            pltpu.VMEM((held + 2 * PAD, width), F32),
            pltpu.VMEM((degree + 1, count, width), F32),
            pltpu.VMEM(((copies + 1) * held, width), BF16),
            pltpu.VMEM(((copies + 1) * held, 2 * width), F32),
            pltpu.VMEM((count, 3 * width), F32),
            pltpu.VMEM((3, count, 3 * width), F32),
            pltpu.VMEM((count, width), F32),
            pltpu.VMEM((count, width), F32),
            pltpu.VMEM((count, width), BF16),
            *[pltpu.VMEM((ROWS, 4 * held), F32)] * 2,
            pltpu.SemaphoreType.DMA((11,)),
            pltpu.SemaphoreType.DMA((7 + copies,)),
            pltpu.SemaphoreType.DMA((7 + copies,)),
            pltpu.SemaphoreType.DMA((count // BIG,)),
        ],
        compiler_params=pltpu.CompilerParams(collective_id=0, has_side_effects=True),
        name="layer",
    )(nodes, clusters, senders, members, wk, wv, wei, weo, wni, wno, gain)


def solution(mesh):
    blocks = ("gx", "gy", "gz")
    in_specs = (P(blocks, None), P(blocks, None), P(blocks, None), P(blocks)) + (P(),) * 7
    return jax.shard_map(
        functools.partial(on_device, mesh),
        mesh=mesh, in_specs=in_specs, out_specs=P(blocks, None), check_vma=False,
    )
```

```python
import functools
import math

import jax
import jax.numpy as jnp
from jax import lax
from jax.experimental import pallas as pl
from jax.experimental.pallas import tpu as pltpu
from jax.sharding import PartitionSpec as P

MESH = pl.DeviceIdType.MESH
F32 = jnp.float32
BF16 = jnp.bfloat16
ROWS = 256
BIG = 512
PAD = 8
NT = (((1,), (1,)), ((), ()))


def dot(a, b):
    return jnp.dot(a, b, preferred_element_type=F32)


def silu(x):
    half = 0.5 * x
    return half * jnp.tanh(half) + half


def kernel(
    nodes_h, clusters_h, senders_h, members_h, wk_h, wv_h, wei_h, weo_h, wni_h, wno_h, gain_h,
    out_h,
    senders, members, nodes, clusters, wk, wv, wei, weo, wni, wno, gain,
    far, faces, table, ctable, planes, keys, values, first, lines, receiver, base, out_v,
    score_a, score_b,
    load_sem, send_sem, recv_sem, out_sem,
):
    count, width = nodes.shape
    held = clusters.shape[0]
    bound = faces.shape[0] // 6
    gx, gy, gz = (lax.axis_index(a) for a in ("gx", "gy", "gz"))
    nx, ny, nz = (lax.axis_size(a) for a in ("gx", "gy", "gz"))
    scale = math.log2(math.e) / math.sqrt(width)

    half = ny_ring = nx // 2
    upper, ring = lax.div(gx, ny_ring), lax.rem(gx, ny_ring)

    core = gy + 1 - 2 * lax.rem(gy, 2)
    side = lax.rem(gy + ny // 2, ny)
    diagonal = lax.rem(core + ny // 2, ny)
    to_gy = {"core": {"gy": core}, "side": {"gy": side}, "diag": {"gy": diagonal}}

    def to_gz(d):
        return {"gz": lax.rem(gz + d % nz, nz)}

    def to_gx(d):
        return {"gx": lax.rem(gx + d % nx, nx)}

    def to_ring(d):
        return {"gx": upper * ny_ring + lax.rem(ring + d % ny_ring, ny_ring)}

    across = {"gx": lax.rem(gx + half, nx)}
    halo = [to_gx(1), to_gx(-1), {"gy": lax.rem(gy + 1, ny)}, {"gy": lax.rem(gy + ny - 1, ny)}, to_gz(1), to_gz(-1)]
    partners = [*to_gy.values()] + [to_gz(d) for d in (1, -1, 2, -2)]
    partners += [across] + [to_ring(d) for d in (1, -1, 2)] + [to_gx(1), to_gx(-1)]

    barrier = pltpu.get_barrier_semaphore()
    for device in partners:
        pl.semaphore_signal(barrier, inc=1, device_id=device, device_id_type=MESH)

    loads = [
        pltpu.make_async_copy(src, dst, load_sem.at[i])
        for i, (src, dst) in enumerate(
            (
                (nodes_h, nodes), (clusters_h, clusters), (wk_h, wk), (wv_h, wv), (wei_h, wei),
                (weo_h, weo), (wni_h, wni), (wno_h, wno), (gain_h, gain), (senders_h, senders),
                (members_h, members),
            )
        )
    ]
    for copy in loads:
        copy.start()
    with jax.named_scope("load_wait"):
        loads[0].wait()
        loads[1].wait()
    with jax.named_scope("barrier_wait"):
        pl.semaphore_wait(barrier, len(partners))

    slots = ["core", "side", "diag", "z-1", "z1", "z-2", "z2", "z-3", "z3", "z4"]
    slots += ["r-1", "r1", "x", "r2", "xr-1", "xr1", "xr2"]
    slot = {name: i for i, name in enumerate(slots)}
    copies = {}

    def send(key, src, dst, device):
        i = len(copies)
        copies[key] = pltpu.make_async_remote_copy(
            src_ref=src, dst_ref=dst, send_sem=send_sem.at[i], recv_sem=recv_sem.at[i],
            device_id=device, device_id_type=MESH,
        )
        copies[key].start()

    def cell(name, start=0, size=held):
        return far.at[pl.ds(slot[name] * held + start, size)]

    border = nodes.at[pl.ds(0, bound)]
    send("core", clusters, cell("core"), to_gy["core"])
    send("x", clusters, cell("x"), across)
    send("z-1", clusters, cell("z-1"), to_gz(1))
    send("z1", clusters, cell("z1"), to_gz(-1))
    send("r-1", clusters, cell("r-1"), to_ring(1))
    send("r1", clusters, cell("r1"), to_ring(-1))
    send("side", clusters, cell("side"), to_gy["side"])
    send("diag", clusters, cell("diag"), to_gy["diag"])
    send("z-2", clusters, cell("z-2"), to_gz(2))
    send("z2", clusters, cell("z2"), to_gz(-2))
    send("h0", border, faces.at[pl.ds(0 * bound, bound)], halo[0])
    send("h1", border, faces.at[pl.ds(1 * bound, bound)], halo[1])
    send("h2", border, faces.at[pl.ds(2 * bound, bound)], halo[2])
    send("h3", border, faces.at[pl.ds(3 * bound, bound)], halo[3])
    send("h4", border, faces.at[pl.ds(4 * bound, bound)], halo[4])
    send("h5", border, faces.at[pl.ds(5 * bound, bound)], halo[5])
    send("r2", clusters, cell("r2"), to_ring(2))

    def arrive(*names):
        for name in names:
            with jax.named_scope("wait_" + name):
                copies[name].wait_recv()

    def relay_x():
        arrive("x")
        for d in (1, -1, 2):
            name = "xr2" if d == 2 else f"xr{-d}"
            send(name, cell("x"), cell(name), to_ring(d))

    def relay_z():
        for sign, start in ((-1, 0), (1, held // 2)):
            here = f"z{2 * sign}"
            arrive(here)
            send(f"z{3 * sign}", cell(here), cell(f"z{3 * sign}"), to_gz(-sign))
            send(f"z4_{start}", cell(here, start, held // 2), cell("z4", start, held // 2), to_gz(-2 * sign))

    for copy in loads[2:]:
        copy.wait()

    w_kv = jnp.concatenate([wk[...], wv[...]], axis=1)
    values[:, pl.ds(width, width)] = jnp.ones((values.shape[0], width), F32)

    def project(block, at, blocks):
        both = dot(block, w_kv)
        rows = pl.ds(at * held, blocks * held)
        keys[rows, :] = both[:, :width].astype(BF16)
        values[rows, pl.ds(0, width)] = both[:, width:].astype(BF16).astype(F32)

    steps = count // ROWS
    score = (score_a, score_b)

    def rows_of(i):
        return pl.ds(i * ROWS, ROWS)

    def scores_of(at, blocks, before, after, i, p):
        reach, near = pl.ds(at * held, blocks * held), pl.ds(0, blocks * held)
        score[p][:, near] = lax.dot_general(nodes[rows_of(i), :], keys[reach, :], NT, preferred_element_type=F32)

    def sums_of(at, blocks, before, after, i, p):
        span = blocks * held
        rows, both = rows_of(i), pl.ds(width, 2 * width)
        scores = score[p][:, pl.ds(0, span)]
        top = jnp.max(scores, axis=1, keepdims=True)
        if before is None:
            top = jnp.broadcast_to(top, (ROWS, width))
        else:
            old = before[rows, pl.ds(0, width)]
            top = jnp.maximum(old, top)
            fade = jnp.exp2((old - top) * scale)
        after[rows, pl.ds(0, width)] = top
        weight = [jnp.exp2((scores[:, g : g + width] - top) * scale) for g in range(0, span, width)]
        gained = dot(jnp.concatenate(weight, axis=1), values[pl.ds(at * held, span), :])
        if before is not None:
            gained = gained + before[rows, both] * jnp.concatenate([fade, fade], axis=1)
        after[rows, both] = gained

    line = []

    def advance(entry):
        n = len(line)
        line.append(entry)
        if entry:
            scores_of(*entry, n % 2)
        if n >= 1:
            sums_of(*line[n - 1], (n - 1) % 2)

    def attend(names, before, after, fill=None):
        first_slot = slot[names[0]] + 1 if names else 0
        blocks = max(len(names), 1)
        if names:
            project(far[pl.ds((first_slot - 1) * held, blocks * held), :], first_slot, blocks)
        else:
            project(clusters[...], 0, 1)
        for i in range(steps):
            advance((first_slot, blocks, before, after, i))
            if fill is not None:
                fill(i)

    own_w, sender_w = pl.ds(0, width), pl.ds(width, width)
    degree = senders.shape[0] * senders.shape[1] // count
    lanes = senders.shape[1]
    part = lanes // degree

    sublane = lax.broadcasted_iota(jnp.int32, (PAD, width), 0)

    def pick_rows(source, places):
        rows = None
        for k, place in enumerate(places):
            loaded = source[pl.ds(place + (PAD - k), PAD), :]
            rows = loaded if rows is None else jnp.where(sublane == k, loaded, rows)
        return rows

    def pick(i):
        for start in range(i * part, i * part + part, PAD):
            ends = range(start, start + PAD)
            for j in range(degree):
                flat = [n * degree + j for n in ends]
                planes[j, pl.ds(start, PAD), :] = pick_rows(table, [senders[f // lanes, f % lanes] for f in flat])

    def pick_own(i, carry):
        start = pl.multiple_of(i * part, part)
        for n in range(0, part, PAD):
            own = pick_rows(ctable, [members[start + n + k] for k in range(PAD)])
            base[pl.ds(start + n, PAD), :] = base[pl.ds(start + n, PAD), :] + own
        return carry

    def picks(begin, each):
        def fill(i):
            for m in range(begin + i * each, begin + i * each + each):
                pick(m)

        return fill

    w_out = weo[...]
    w_outs = jnp.concatenate([w_out] * degree, axis=0)

    def edges(i):
        rows = rows_of(i)
        to = receiver[rows, :]
        hidden = jnp.concatenate([silu(planes[j, rows, :] + to).astype(BF16) for j in range(degree)], axis=1)
        aggregated = dot(hidden, w_outs).astype(BF16)
        base[rows, :] = base[rows, :] + dot(aggregated, wni[pl.ds(width, width), :])

    attend((), None, first)
    table[pl.ds(PAD, count), :] = dot(nodes[...], wei[sender_w, :])
    receiver[...] = dot(nodes[...], wei[own_w, :])
    for padded in (table, ctable):
        padded[pl.ds(0, PAD), :] = jnp.zeros((PAD, width), F32)
        padded[pl.ds(padded.shape[0] - PAD, PAD), :] = jnp.zeros((PAD, width), F32)
    ctable[pl.ds(PAD, held), :] = dot(clusters[...], wni[pl.ds(3 * width, width), :])
    base[...] = dot(nodes[...], wni[pl.ds(0, width), :])
    arrive("core")
    attend(("core",), first, lines.at[0])
    with jax.named_scope("members"):
        lax.fori_loop(0, count // part, pick_own, 0)
    arrive("z-1", "z1")
    attend(("z-1", "z1"), first, lines.at[1])
    relay_x()
    arrive("r-1", "r1")
    attend(("r-1", "r1"), first, lines.at[2])
    arrive("side", "diag")
    attend(("side", "diag"), lines.at[0], lines.at[0])
    relay_z()
    attend(("z-2", "z2"), lines.at[1], lines.at[1])
    for i in range(len(halo)):
        arrive(f"h{i}")
    table[pl.ds(PAD + count, 6 * bound), :] = dot(faces[...], wei[sender_w, :])
    each = senders.shape[0] // (2 * steps)
    arrive("r2")
    attend(("x", "r2"), lines.at[2], lines.at[2], picks(0, each))
    arrive("xr-1", "xr1", "xr2")
    attend(("xr-1", "xr1", "xr2"), lines.at[2], lines.at[2], picks(steps * each, each))
    arrive("z-3", "z3", "z4_0", f"z4_{held // 2}")
    attend(("z-3", "z3", "z4"), lines.at[1], lines.at[1], edges)
    advance(None)

    eps_pool, eps_norm = 1e-06, 1e-05

    def finish(i, carry):
        rows = pl.ds(i * BIG, BIG)
        pooled = jnp.zeros((BIG, width), F32)
        for which in range(3):
            pooled = pooled + lines[which, rows, pl.ds(width, width)] / lines[which, rows, pl.ds(2 * width, width)]
        attended = (pooled * lax.rsqrt(jnp.mean(pooled * pooled, axis=1, keepdims=True) + eps_pool)).astype(BF16)
        preact = dot(attended, wni[pl.ds(2 * width, width), :]) + base[rows, :]
        update = dot(silu(preact).astype(BF16), wno[...])
        centred = update - jnp.mean(update, axis=1, keepdims=True)
        variance = jnp.mean(centred * centred, axis=1, keepdims=True)
        normed = centred * lax.rsqrt(variance + eps_norm)
        out_v[rows, :] = (nodes[rows, :].astype(F32) + normed * gain[...]).astype(BF16)
        return carry

    pieces = []
    with jax.named_scope("finish"):
        for i in range(count // BIG):
            finish(i, 0)
            rows = pl.ds(i * BIG, BIG)
            pieces.append(pltpu.make_async_copy(out_v.at[rows], out_h.at[rows], out_sem.at[i]))
            pieces[-1].start()
    with jax.named_scope("end"):
        for sent in copies.values():
            sent.wait_send()
        for copy in pieces:
            copy.wait()


def on_device(mesh, *args):
    nodes, clusters, senders, members, wk, wv, wei, weo, wni, wno, gain = args
    count, width = nodes.shape
    held = clusters.shape[0]
    bound = count // 2
    copies = sum(mesh.shape[a] - 1 for a in ("gx", "gy", "gz"))
    degree = senders.size // count
    hbm = pl.BlockSpec(memory_space=pl.ANY)
    vmem = lambda a: pltpu.VMEM(a.shape, a.dtype)
    gain = gain.reshape(1, width)
    return pl.pallas_call(
        kernel,
        out_shape=jax.ShapeDtypeStruct((count, width), BF16),
        in_specs=[hbm] * 11,
        out_specs=hbm,
        scratch_shapes=[
            pltpu.SMEM(senders.shape, senders.dtype),
            pltpu.SMEM(members.shape, members.dtype),
            *(vmem(a) for a in (nodes, clusters, wk, wv, wei, weo, wni, wno, gain)),
            pltpu.VMEM((copies * held, width), BF16),
            pltpu.VMEM((6 * bound, width), BF16),
            pltpu.VMEM((count + 6 * bound + 2 * PAD, width), F32),
            pltpu.VMEM((held + 2 * PAD, width), F32),
            pltpu.VMEM((degree, count, width), F32),
            pltpu.VMEM(((copies + 1) * held, width), BF16),
            pltpu.VMEM(((copies + 1) * held, 2 * width), F32),
            pltpu.VMEM((count, 3 * width), F32),
            pltpu.VMEM((3, count, 3 * width), F32),
            pltpu.VMEM((count, width), F32),
            pltpu.VMEM((count, width), F32),
            pltpu.VMEM((count, width), BF16),
            *[pltpu.VMEM((ROWS, 4 * held), F32)] * 2,
            pltpu.SemaphoreType.DMA((11,)),
            pltpu.SemaphoreType.DMA((7 + copies,)),
            pltpu.SemaphoreType.DMA((7 + copies,)),
            pltpu.SemaphoreType.DMA((count // BIG,)),
        ],
        compiler_params=pltpu.CompilerParams(collective_id=0, has_side_effects=True),
        name="layer",
    )(nodes, clusters, senders, members, wk, wv, wei, weo, wni, wno, gain)


def solution(mesh):
    blocks = ("gx", "gy", "gz")
    in_specs = (P(blocks, None), P(blocks, None), P(blocks, None), P(blocks)) + (P(),) * 7
    return jax.shard_map(
        functools.partial(on_device, mesh),
        mesh=mesh, in_specs=in_specs, out_specs=P(blocks, None), check_vma=False,
    )
```

```python
import functools
import math

import jax
import jax.numpy as jnp
from jax import lax
from jax.experimental import pallas as pl
from jax.experimental.pallas import tpu as pltpu
from jax.sharding import PartitionSpec as P

MESH = pl.DeviceIdType.MESH
F32 = jnp.float32
BF16 = jnp.bfloat16
ROWS = 256
BIG = 512
PAD = 8
NT = (((1,), (1,)), ((), ()))


def dot(a, b):
    return jnp.dot(a, b, preferred_element_type=F32)


def silu(x):
    half = 0.5 * x
    return half * jnp.tanh(half) + half


def kernel(
    nodes_h, clusters_h, senders_h, members_h, wk_h, wv_h, wei_h, weo_h, wni_h, wno_h, gain_h,
    out_h,
    senders, members, nodes, clusters, wk, wv, wei, weo, wni, wno, gain,
    far, faces, table, ctable, planes, keys, values, first, lines, receiver, base, out_v,
    score_a, score_b,
    load_sem, send_sem, recv_sem, out_sem,
):
    count, width = nodes.shape
    held = clusters.shape[0]
    bound = faces.shape[0] // 6
    gx, gy, gz = (lax.axis_index(a) for a in ("gx", "gy", "gz"))
    nx, ny, nz = (lax.axis_size(a) for a in ("gx", "gy", "gz"))
    scale = math.log2(math.e) / math.sqrt(width)

    half = ny_ring = nx // 2
    upper, ring = lax.div(gx, ny_ring), lax.rem(gx, ny_ring)

    core = gy + 1 - 2 * lax.rem(gy, 2)
    side = lax.rem(gy + ny // 2, ny)
    diagonal = lax.rem(core + ny // 2, ny)
    to_gy = {"core": {"gy": core}, "side": {"gy": side}, "diag": {"gy": diagonal}}

    def to_gz(d):
        return {"gz": lax.rem(gz + d % nz, nz)}

    def to_gx(d):
        return {"gx": lax.rem(gx + d % nx, nx)}

    def to_ring(d):
        return {"gx": upper * ny_ring + lax.rem(ring + d % ny_ring, ny_ring)}

    across = {"gx": lax.rem(gx + half, nx)}
    halo = [to_gx(1), to_gx(-1), {"gy": lax.rem(gy + 1, ny)}, {"gy": lax.rem(gy + ny - 1, ny)}, to_gz(1), to_gz(-1)]
    partners = [*to_gy.values()] + [to_gz(d) for d in (1, -1, 2, -2)]
    partners += [across] + [to_ring(d) for d in (1, -1, 2)] + [to_gx(1), to_gx(-1)]

    barrier = pltpu.get_barrier_semaphore()
    for device in partners:
        pl.semaphore_signal(barrier, inc=1, device_id=device, device_id_type=MESH)

    loads = [
        pltpu.make_async_copy(src, dst, load_sem.at[i])
        for i, (src, dst) in enumerate(
            (
                (nodes_h, nodes), (clusters_h, clusters), (wk_h, wk), (wv_h, wv), (wei_h, wei),
                (weo_h, weo), (wni_h, wni), (wno_h, wno), (gain_h, gain), (senders_h, senders),
                (members_h, members),
            )
        )
    ]
    for copy in loads:
        copy.start()
    with jax.named_scope("load_wait"):
        loads[0].wait()
        loads[1].wait()
    with jax.named_scope("barrier_wait"):
        pl.semaphore_wait(barrier, len(partners))

    slots = ["core", "side", "diag", "z-1", "z1", "z-2", "z2", "z-3", "z3", "z4"]
    slots += ["r-1", "r1", "x", "r2", "xr-1", "xr1", "xr2"]
    slot = {name: i for i, name in enumerate(slots)}
    copies = {}

    def send(key, src, dst, device):
        i = len(copies)
        copies[key] = pltpu.make_async_remote_copy(
            src_ref=src, dst_ref=dst, send_sem=send_sem.at[i], recv_sem=recv_sem.at[i],
            device_id=device, device_id_type=MESH,
        )
        copies[key].start()

    def cell(name, start=0, size=held):
        return far.at[pl.ds(slot[name] * held + start, size)]

    border = nodes.at[pl.ds(0, bound)]
    send("core", clusters, cell("core"), to_gy["core"])
    send("x", clusters, cell("x"), across)
    send("z-1", clusters, cell("z-1"), to_gz(1))
    send("z1", clusters, cell("z1"), to_gz(-1))
    send("r-1", clusters, cell("r-1"), to_ring(1))
    send("r1", clusters, cell("r1"), to_ring(-1))
    send("side", clusters, cell("side"), to_gy["side"])
    send("diag", clusters, cell("diag"), to_gy["diag"])
    send("z-2", clusters, cell("z-2"), to_gz(2))
    send("z2", clusters, cell("z2"), to_gz(-2))
    send("h0", border, faces.at[pl.ds(0 * bound, bound)], halo[0])
    send("h1", border, faces.at[pl.ds(1 * bound, bound)], halo[1])
    send("h2", border, faces.at[pl.ds(2 * bound, bound)], halo[2])
    send("h3", border, faces.at[pl.ds(3 * bound, bound)], halo[3])
    send("h4", border, faces.at[pl.ds(4 * bound, bound)], halo[4])
    send("h5", border, faces.at[pl.ds(5 * bound, bound)], halo[5])
    send("r2", clusters, cell("r2"), to_ring(2))

    def arrive(*names):
        for name in names:
            with jax.named_scope("wait_" + name):
                copies[name].wait_recv()

    def relay_x():
        arrive("x")
        for d in (1, -1, 2):
            name = "xr2" if d == 2 else f"xr{-d}"
            send(name, cell("x"), cell(name), to_ring(d))

    def relay_z():
        for sign, start in ((-1, 0), (1, held // 2)):
            here = f"z{2 * sign}"
            arrive(here)
            send(f"z{3 * sign}", cell(here), cell(f"z{3 * sign}"), to_gz(-sign))
            send(f"z4_{start}", cell(here, start, held // 2), cell("z4", start, held // 2), to_gz(-2 * sign))

    for copy in loads[2:]:
        copy.wait()

    w_kv = jnp.concatenate([wk[...], wv[...]], axis=1)
    values[:, pl.ds(width, width)] = jnp.ones((values.shape[0], width), F32)

    def project(block, at, blocks):
        both = dot(block, w_kv)
        rows = pl.ds(at * held, blocks * held)
        keys[rows, :] = both[:, :width].astype(BF16)
        values[rows, pl.ds(0, width)] = both[:, width:].astype(BF16).astype(F32)

    steps = count // ROWS
    score = (score_a, score_b)

    def rows_of(i):
        return pl.ds(i * ROWS, ROWS)

    def scores_of(at, blocks, before, after, i, p):
        reach, near = pl.ds(at * held, blocks * held), pl.ds(0, blocks * held)
        score[p][:, near] = lax.dot_general(nodes[rows_of(i), :], keys[reach, :], NT, preferred_element_type=F32)

    def sums_of(at, blocks, before, after, i, p):
        span = blocks * held
        rows, both = rows_of(i), pl.ds(width, 2 * width)
        scores = score[p][:, pl.ds(0, span)]
        top = jnp.max(scores, axis=1, keepdims=True)
        if before is None:
            top = jnp.broadcast_to(top, (ROWS, width))
        else:
            old = before[rows, pl.ds(0, width)]
            top = jnp.maximum(old, top)
            fade = jnp.exp2((old - top) * scale)
        after[rows, pl.ds(0, width)] = top
        weight = [jnp.exp2((scores[:, g : g + width] - top) * scale) for g in range(0, span, width)]
        gained = dot(jnp.concatenate(weight, axis=1), values[pl.ds(at * held, span), :])
        if before is not None:
            gained = gained + before[rows, both] * jnp.concatenate([fade, fade], axis=1)
        after[rows, both] = gained

    line = []

    def advance(entry):
        n = len(line)
        line.append(entry)
        if entry:
            scores_of(*entry, n % 2)
        if n >= 1:
            sums_of(*line[n - 1], (n - 1) % 2)

    def attend(names, before, after, fill=None):
        first_slot = slot[names[0]] + 1 if names else 0
        blocks = max(len(names), 1)
        if names:
            project(far[pl.ds((first_slot - 1) * held, blocks * held), :], first_slot, blocks)
        else:
            project(clusters[...], 0, 1)
        for i in range(steps):
            advance((first_slot, blocks, before, after, i))
            if fill is not None:
                fill(i)

    own_w, sender_w = pl.ds(0, width), pl.ds(width, width)
    degree = senders.shape[0] * senders.shape[1] // count
    lanes = senders.shape[1]
    part = lanes // degree

    sublane = lax.broadcasted_iota(jnp.int32, (PAD, width), 0)

    def pick_rows(source, places):
        rows = None
        for k, place in enumerate(places):
            loaded = source[pl.ds(place + (PAD - k), PAD), :]
            rows = loaded if rows is None else jnp.where(sublane == k, loaded, rows)
        return rows

    def pick(i):
        for start in range(i * part, i * part + part, PAD):
            ends = range(start, start + PAD)
            for j in range(degree):
                flat = [n * degree + j for n in ends]
                planes[j, pl.ds(start, PAD), :] = pick_rows(table, [senders[f // lanes, f % lanes] for f in flat])

    def pick_own(i, carry):
        start = pl.multiple_of(i * part, part)
        for n in range(0, part, PAD):
            own = pick_rows(ctable, [members[start + n + k] for k in range(PAD)])
            base[pl.ds(start + n, PAD), :] = base[pl.ds(start + n, PAD), :] + own
        return carry

    def picks(begin, each):
        def fill(i):
            for m in range(begin + i * each, begin + i * each + each):
                pick(m)

        return fill

    w_out = weo[...]
    w_outs = jnp.concatenate([w_out] * degree, axis=0)

    def edges(i):
        rows = rows_of(i)
        to = receiver[rows, :]
        hidden = jnp.concatenate([silu(planes[j, rows, :] + to).astype(BF16) for j in range(degree)], axis=1)
        aggregated = dot(hidden, w_outs).astype(BF16)
        base[rows, :] = base[rows, :] + dot(aggregated, wni[pl.ds(width, width), :])

    attend((), None, first)
    table[pl.ds(PAD, count), :] = dot(nodes[...], wei[sender_w, :])
    receiver[...] = dot(nodes[...], wei[own_w, :])
    for padded in (table, ctable):
        padded[pl.ds(0, PAD), :] = jnp.zeros((PAD, width), F32)
        padded[pl.ds(padded.shape[0] - PAD, PAD), :] = jnp.zeros((PAD, width), F32)
    ctable[pl.ds(PAD, held), :] = dot(clusters[...], wni[pl.ds(3 * width, width), :])
    base[...] = dot(nodes[...], wni[pl.ds(0, width), :])
    arrive("core")
    attend(("core",), first, lines.at[0])
    with jax.named_scope("members"):
        lax.fori_loop(0, count // part, pick_own, 0)
    arrive("z-1", "z1")
    attend(("z-1", "z1"), first, lines.at[1])
    relay_x()
    arrive("r-1", "r1")
    attend(("r-1", "r1", "x"), first, lines.at[2])
    arrive("side", "diag")
    attend(("side", "diag"), lines.at[0], lines.at[0])
    relay_z()
    attend(("z-2", "z2"), lines.at[1], lines.at[1])
    for i in range(len(halo)):
        arrive(f"h{i}")
    table[pl.ds(PAD + count, 6 * bound), :] = dot(faces[...], wei[sender_w, :])
    for i in range(senders.shape[0]):
        pick(i)
    for i in range(steps):
        edges(i)
    arrive("r2", "xr-1", "xr1", "xr2")
    attend(("r2", "xr-1", "xr1", "xr2"), lines.at[2], lines.at[2])
    arrive("z-3", "z3", "z4_0", f"z4_{held // 2}")
    attend(("z-3", "z3", "z4"), lines.at[1], lines.at[1])
    advance(None)

    eps_pool, eps_norm = 1e-06, 1e-05

    def finish(i, carry):
        rows = pl.ds(i * BIG, BIG)
        pooled = jnp.zeros((BIG, width), F32)
        for which in range(3):
            pooled = pooled + lines[which, rows, pl.ds(width, width)] / lines[which, rows, pl.ds(2 * width, width)]
        attended = (pooled * lax.rsqrt(jnp.mean(pooled * pooled, axis=1, keepdims=True) + eps_pool)).astype(BF16)
        preact = dot(attended, wni[pl.ds(2 * width, width), :]) + base[rows, :]
        update = dot(silu(preact).astype(BF16), wno[...])
        centred = update - jnp.mean(update, axis=1, keepdims=True)
        variance = jnp.mean(centred * centred, axis=1, keepdims=True)
        normed = centred * lax.rsqrt(variance + eps_norm)
        out_v[rows, :] = (nodes[rows, :].astype(F32) + normed * gain[...]).astype(BF16)
        return carry

    pieces = []
    with jax.named_scope("finish"):
        for i in range(count // BIG):
            finish(i, 0)
            rows = pl.ds(i * BIG, BIG)
            pieces.append(pltpu.make_async_copy(out_v.at[rows], out_h.at[rows], out_sem.at[i]))
            pieces[-1].start()
    with jax.named_scope("end"):
        for sent in copies.values():
            sent.wait_send()
        for copy in pieces:
            copy.wait()


def on_device(mesh, *args):
    nodes, clusters, senders, members, wk, wv, wei, weo, wni, wno, gain = args
    count, width = nodes.shape
    held = clusters.shape[0]
    bound = count // 2
    copies = sum(mesh.shape[a] - 1 for a in ("gx", "gy", "gz"))
    degree = senders.size // count
    hbm = pl.BlockSpec(memory_space=pl.ANY)
    vmem = lambda a: pltpu.VMEM(a.shape, a.dtype)
    gain = gain.reshape(1, width)
    return pl.pallas_call(
        kernel,
        out_shape=jax.ShapeDtypeStruct((count, width), BF16),
        in_specs=[hbm] * 11,
        out_specs=hbm,
        scratch_shapes=[
            pltpu.SMEM(senders.shape, senders.dtype),
            pltpu.SMEM(members.shape, members.dtype),
            *(vmem(a) for a in (nodes, clusters, wk, wv, wei, weo, wni, wno, gain)),
            pltpu.VMEM((copies * held, width), BF16),
            pltpu.VMEM((6 * bound, width), BF16),
            pltpu.VMEM((count + 6 * bound + 2 * PAD, width), F32),
            pltpu.VMEM((held + 2 * PAD, width), F32),
            pltpu.VMEM((degree, count, width), F32),
            pltpu.VMEM(((copies + 1) * held, width), BF16),
            pltpu.VMEM(((copies + 1) * held, 2 * width), F32),
            pltpu.VMEM((count, 3 * width), F32),
            pltpu.VMEM((3, count, 3 * width), F32),
            pltpu.VMEM((count, width), F32),
            pltpu.VMEM((count, width), F32),
            pltpu.VMEM((count, width), BF16),
            *[pltpu.VMEM((ROWS, 4 * held), F32)] * 2,
            pltpu.SemaphoreType.DMA((11,)),
            pltpu.SemaphoreType.DMA((7 + copies,)),
            pltpu.SemaphoreType.DMA((7 + copies,)),
            pltpu.SemaphoreType.DMA((count // BIG,)),
        ],
        compiler_params=pltpu.CompilerParams(collective_id=0, has_side_effects=True),
        name="layer",
    )(nodes, clusters, senders, members, wk, wv, wei, weo, wni, wno, gain)


def solution(mesh):
    blocks = ("gx", "gy", "gz")
    in_specs = (P(blocks, None), P(blocks, None), P(blocks, None), P(blocks)) + (P(),) * 7
    return jax.shard_map(
        functools.partial(on_device, mesh),
        mesh=mesh, in_specs=in_specs, out_specs=P(blocks, None), check_vma=False,
    )
```
